32 devices in a mesh: tok: 8 (over y, x, core), slot: 4 (over z).
Axes of the slice: x: 2, y: 2, z: 4, core: 2. Of those that a mesh axis runs over, the one named last changes fastest.
Arguments:
- tokens: bfloat16 [8192, 1024], P('tok'), may hold values from -16 to 16
- slot_params: bfloat16 [8192, 1024], P('slot'), may hold values from -0.5 to 0.5
- w_in: bfloat16 [16, 1024, 4096], P('slot', None, 'tok'), may hold values from -0.1875 to 0.1875
- w_out: bfloat16 [16, 4096, 1024], P('slot', 'tok'), may hold values from -0.09375 to 0.09375
Outputs:
- mixed: bfloat16 [8192, 1024], P(('tok', 'slot'))
The draws below stay inside these ranges and needn't reach their ends.
All inputs are finite; a program needn't handle non-finite values.
Results may differ from the reference program's by a relative error of at most 0.01.
Values may be sent and summed in bfloat16 or wider, within the bound.
No kernel may reach another device: no remote copies, remote signals or barrier semaphores. Data moves between devices by JAX's collectives and lax.ppermute only.
A program may use at most 64 MiB of HBM per device.

```python
import math
import jax
import jax.numpy as jnp
from jax import lax

D = 1024
H = 4096
P_SIZE = 8
EXP_COL = 4
TOKENS = 8192
SLOTS = 8192
SLOT_COL = 2048
EXPERTS = 16


def slot_table(key):
    raw = jax.random.normal(jax.random.fold_in(key, 11), (SLOTS, D), jnp.float32)
    return jnp.clip(raw * (3.0 / math.sqrt(D)), -0.5, 0.5)


def draw_slot_params(key, part):
    return slot_table(key).astype(jnp.bfloat16)


def draw_tokens(key, part):
    base = jax.random.normal(jax.random.fold_in(key, 23), (TOKENS, D), jnp.float32)
    return jnp.clip(base, -5.0, 5.0).astype(jnp.bfloat16)


def shard_levels(key, shape, shards, smallest, high):
    def one(position, parts):
        steps = jax.random.uniform(jax.random.fold_in(jax.random.fold_in(key, 6), position), (parts,), jnp.float32, smallest / len(shards), high / len(shards))
        return jnp.repeat(jnp.exp(steps), shape[position] // parts).reshape((-1,) + (1,) * (len(shape) - position - 1))

    loudness = one(*shards[0])
    for cut in shards[1:]:
        loudness = loudness * one(*cut)
    return loudness


def gaussian(key, extent, width, most, cuts=(), held_as=jnp.bfloat16):
    result = jax.random.normal(key, extent, jnp.float32) * width
    if len(cuts) > 0:
        result = shard_levels(key, extent, cuts, -0.22, 0.18) * result
    return jnp.clip(result, min=-most, max=most).astype(held_as)


def setup_inputs(seed: int = 0) -> dict:
    keys = jax.random.split(jax.random.key(seed), 5)
    return {
        "tokens": draw_tokens(jax.random.fold_in(keys[4], 71), 0),
        "slot_params": draw_slot_params(jax.random.fold_in(keys[4], 71), 0),
        "w_in": gaussian(keys[2], (EXPERTS, D, H), D ** -0.5, 0.1875, ((0, 4), (2, 8))),
        "w_out": gaussian(keys[3], (EXPERTS, H, D), H ** -0.5, 0.09375, ((0, 4), (1, 8))),
    }


def reference(tokens, slot_params, w_in, w_out):
    logits = lax.dot_general(slot_params, tokens, (((1,), (1,)), ((), ())), preferred_element_type=jnp.float32)
    row_index = jnp.arange(EXPERTS * P_SIZE, dtype=jnp.int32)
    expert = row_index // P_SIZE
    within = row_index % P_SIZE
    chosen = ((expert // EXP_COL) * SLOT_COL + (expert % EXP_COL) * P_SIZE + within).astype(jnp.int32)
    flight = jnp.take(logits, chosen, axis=0)
    col_max = jnp.max(flight, axis=1, keepdims=True)
    dispatch_exp = jnp.exp(flight - col_max)
    dispatch_w = dispatch_exp.astype(jnp.bfloat16)
    totals = jnp.sum(dispatch_exp, axis=1, keepdims=True)
    numer = jnp.dot(dispatch_w, tokens, preferred_element_type=jnp.float32)
    slot_in = (numer / totals).astype(jnp.bfloat16).reshape(EXPERTS, P_SIZE, D)

    def expert_mlp(packed):
        vectors, first, second = packed
        pre_act = jnp.dot(vectors, first, preferred_element_type=jnp.float32)
        hidden = jax.nn.gelu(pre_act).astype(jnp.bfloat16)
        return jnp.dot(hidden, second, preferred_element_type=jnp.float32).astype(jnp.bfloat16)

    slot_out = lax.map(expert_mlp, (slot_in, w_in, w_out)).reshape(EXPERTS * P_SIZE, D)
    row_max = jnp.max(logits, axis=0, keepdims=True)
    row_sum = jnp.sum(jnp.exp(logits - row_max), axis=0, keepdims=True)
    combine_w = (jnp.exp(flight - row_max) / row_sum).astype(jnp.bfloat16)
    mixed = lax.dot_general(combine_w, slot_out, (((0,), (0,)), ((), ())), preferred_element_type=jnp.float32)
    return mixed.astype(jnp.bfloat16)
```

```python
import functools

import jax
import jax.numpy as jnp
from jax import lax
from jax.experimental import pallas as pl
from jax.experimental.pallas import tpu as pltpu
from jax.sharding import PartitionSpec as P

P_SIZE = 8
LANES = 128
BF = jnp.bfloat16
F32 = jnp.float32
VMEM = pl.BlockSpec(memory_space=pltpu.VMEM)
SMEM = pl.BlockSpec(memory_space=pltpu.SMEM)


def sds(shape, dtype):
    return jax.ShapeDtypeStruct(shape, dtype)


def call(kernel, outs, n_in, name, flops=0, vmem=None, scalars=0, **kw):
    return pl.pallas_call(
        kernel,
        out_shape=outs,
        in_specs=kw.pop("in_specs", [SMEM] * scalars + [VMEM] * n_in),
        out_specs=jax.tree.map(lambda _: VMEM, outs),
        name=name,
        compiler_params=pltpu.CompilerParams(vmem_limit_bytes=vmem),
        cost_estimate=pl.CostEstimate(flops=flops, bytes_accessed=0, transcendentals=0),
        **kw,
    )


def lane_pack(rows, *columns):
    lane = lax.broadcasted_iota(jnp.int32, (rows, LANES), 1)
    out = jnp.zeros((rows, LANES), F32)
    for k, column in enumerate(columns):
        out = jnp.where(lane == k, column, out)
    return out


def write_state(num, top, tot, num_ref, st_ref, msg_ref):
    rows, d = num.shape
    num_ref[...] = num
    st_ref[...] = lane_pack(rows, top, tot)
    hi = tot.astype(BF).astype(F32)
    lo = (tot - hi).astype(BF).astype(F32)
    msg_ref[:, :d] = num.astype(BF)
    msg_ref[:, d:] = lane_pack(rows, top, hi, lo).astype(BF)


def dispatch_kernel(sp_ref, tok_ref, flight_ref, num_ref, st_ref, msg_ref):
    tok = tok_ref[...]
    flight = lax.dot_general(sp_ref[...], tok, (((1,), (1,)), ((), ())), preferred_element_type=F32)
    flight_ref[...] = flight
    top = jnp.max(flight, axis=1, keepdims=True).astype(BF).astype(F32)
    e = jnp.exp(flight - top)
    tot = jnp.sum(e, axis=1, keepdims=True)
    num = jnp.dot(e.astype(BF), tok, preferred_element_type=F32)
    write_state(num, top, tot, num_ref, st_ref, msg_ref)


def merge(num_ref, st_ref, recv_ref):
    d = num_ref.shape[1]
    top, tot = st_ref[:, 0:1], st_ref[:, 1:2]
    rs = recv_ref[:, d:].astype(F32)
    rtop, rtot = rs[:, 0:1], rs[:, 1:2] + rs[:, 2:3]
    new = jnp.maximum(top, rtop)
    a, b = jnp.exp(top - new), jnp.exp(rtop - new)
    num = num_ref[...] * a + recv_ref[:, :d].astype(F32) * b
    return num, new, tot * a + rtot * b


def merge_kernel(num_ref, st_ref, recv_ref, num_out, st_out, msg_out):
    write_state(*merge(num_ref, st_ref, recv_ref), num_out, st_out, msg_out)


def merge_last_kernel(num_ref, st_ref, recv_ref, out_ref):
    num, _, tot = merge(num_ref, st_ref, recv_ref)
    out_ref[...] = (num / tot).astype(BF)


def mlp_kernel(north_ref, own_ref, recv_ref, win_ref, wout_ref, out_ref, msg_ref):
    x = jnp.where(north_ref[0] == 1, own_ref[...].astype(F32), recv_ref[...].astype(F32))
    experts = win_ref.shape[0]
    for e in range(experts):
        rows = slice(e * P_SIZE, (e + 1) * P_SIZE)
        pre = jnp.dot(x[rows].astype(BF), win_ref[e], preferred_element_type=F32)
        hidden = jax.nn.gelu(pre).astype(BF)
        out_ref[rows, :] = jnp.dot(hidden, wout_ref[e], preferred_element_type=F32)
    msg_ref[...] = out_ref[...].astype(BF)


def stats_kernel(first, step, sp_ref, tok_ref, m_ref, l_ref, mo_ref, lo_ref):
    rows, n = sp_ref.shape[0], tok_ref.shape[0]
    if first:
        m, l = jnp.full((8, n), -jnp.inf, F32), jnp.zeros((8, n), F32)
    else:
        m, l = m_ref[...], l_ref[...]
    tok = tok_ref[...]
    for r in range(0, rows, step):
        x = lax.dot_general(
            sp_ref[r : r + step, :], tok, (((1,), (1,)), ((), ())), preferred_element_type=F32
        ).reshape(step // 8, 8, n)
        new = jnp.maximum(m, jnp.max(x, axis=0))
        l = l * jnp.exp(m - new) + jnp.sum(jnp.exp(x - new[None]), axis=0)
        m = new
    mo_ref[...] = m
    lo_ref[...] = l


def pack_kernel(flight_ref, m_ref, l_ref, out_ref):
    rows = flight_ref.shape[0]
    m, l = m_ref[...], l_ref[...]
    top = jnp.max(m, axis=0, keepdims=True)
    tot = jnp.sum(l * jnp.exp(m - top), axis=0, keepdims=True)
    out_ref[:rows, :] = flight_ref[...]
    sub = lax.broadcasted_iota(jnp.int32, m.shape, 0)
    out_ref[rows:, :] = jnp.where(sub == 0, top, jnp.where(sub == 1, tot, 0.0))


def weights_kernel(*refs):
    parts, out_ref = refs[:-1], refs[-1]
    rows = parts[0].shape[0] - 8
    tops = [p[rows : rows + 1, :] for p in parts]
    top = functools.reduce(jnp.maximum, tops)
    tot = sum(p[rows + 1 : rows + 2, :] * jnp.exp(t - top) for p, t in zip(parts, tops))
    w = jnp.concatenate([jnp.exp(p[:rows, :] - top) / tot for p in parts], axis=0)
    out_ref[...] = w.T.astype(BF)


def combine_kernel(pieces, north_ref, w_ref, *refs):
    own, recv, out_ref = refs[:pieces], refs[pieces : 2 * pieces], refs[2 * pieces]
    scratch = refs[2 * pieces + 1]
    at = 0
    for a, b in zip(own, recv):
        n = a.shape[0]
        scratch[at : at + n, :] = jnp.where(north_ref[0] == 1, a[...], b[...])
        at += n
    out_ref[...] = jnp.dot(w_ref[...], scratch[...], preferred_element_type=F32).astype(BF)


def body(n_tok, n_slot, tokens, slot_params, w_in, w_out):
    n, d = tokens.shape
    experts, _, h = w_in.shape
    rows = experts * P_SIZE
    me_slot = lax.axis_index("slot")
    odd = lax.rem(lax.axis_index("tok"), 2)
    north = odd.astype(jnp.int32).reshape(1)

    def up(x):
        return lax.ppermute(x, "tok", [(i, i + 1) for i in range(0, n_tok, 2)])

    def down(x):
        return lax.ppermute(x, "tok", [(i + 1, i) for i in range(0, n_tok, 2)])

    def swap_tok(x, bit):
        return lax.ppermute(x, "tok", [(i, i ^ bit) for i in range(1, n_tok, 2)])

    def swap_slot(x, bit):
        pairs = [(i * n_slot + j, i * n_slot + (j ^ bit)) for i in range(1, n_tok, 2) for j in range(n_slot)]
        return lax.ppermute(x, ("tok", "slot"), pairs)

    tok_bits = [1 << b for b in range(1, n_tok.bit_length() - 1)]
    slot_bits = [1 << b for b in range(n_slot.bit_length() - 1)]

    state = [sds((rows, d), F32), sds((rows, LANES), F32), sds((rows, d + LANES), BF)]
    flight, num, st, msg = call(
        dispatch_kernel, [sds((rows, n), F32)] + state, 2, "dispatch", flops=4 * rows * n * d, vmem=8 << 20
    )(slot_params[:rows], tokens)
    recv = up(msg)
    for bit in tok_bits:
        num, st, msg = call(merge_kernel, state, 3, "merge", vmem=2 << 20)(num, st, recv)
        recv = swap_tok(msg, bit)
    slot_in = call(merge_last_kernel, sds((rows, d), BF), 3, "merge_last", vmem=2 << 20)(num, st, recv)
    recv = down(slot_in)

    slots = slot_params.shape[0]
    chunk = min(512, slots)
    m = jnp.zeros((8, n), F32)
    l = m
    for c in range(0, slots, chunk):
        m, l = call(
            functools.partial(stats_kernel, c == 0, min(256, chunk)),
            [sds((8, n), F32)] * 2,
            4,
            "stats",
            flops=2 * chunk * n * d,
            vmem=12 << 20,
            grid=(1,),
            in_specs=[
                pl.BlockSpec((chunk, d), lambda i, c=c: (c // chunk, 0)),
                VMEM,
                VMEM,
                VMEM,
            ],
        )(slot_params, tokens, m, l)
    pack = call(pack_kernel, sds((rows + 8, n), F32), 3, "pack", vmem=2 << 20)(flight, m, l)
    share = n // n_slot
    parts = []
    for k in range(n_slot):
        part = lax.dynamic_slice_in_dim(pack, (me_slot ^ k) * share, share, axis=1)
        if k:
            part = lax.ppermute(part, "slot", [(j, j ^ k) for j in range(n_slot)])
        parts.append(part)
    weights = call(weights_kernel, sds((share, n_slot * rows), BF), n_slot, "weights", vmem=4 << 20)(*parts)

    out, msg = call(
        mlp_kernel,
        [sds((rows, d), F32), sds((rows, d), BF)],
        4,
        "mlp",
        flops=4 * rows * d * h,
        vmem=12 << 20,
        scalars=1,
    )(north, slot_in, recv, w_in, w_out)
    out = out + up(msg).astype(F32)
    for bit in tok_bits:
        out = out + swap_tok(out.astype(BF), bit).astype(F32)
    own = [out.astype(BF)]
    for bit in slot_bits:
        have = own[0] if len(own) == 1 else jnp.concatenate(own, axis=0)
        own.append(swap_slot(have, bit))
    below = [down(x) for x in own]
    return pl.pallas_call(
        functools.partial(combine_kernel, len(own)),
        out_shape=sds((share, d), BF),
        in_specs=[SMEM] + [VMEM] * (1 + 2 * len(own)),
        out_specs=VMEM,
        scratch_shapes=[pltpu.VMEM((n_slot * rows, d), BF)],
        name="combine",
        compiler_params=pltpu.CompilerParams(vmem_limit_bytes=8 << 20),
    )(north, weights, *own, *below)


def solution(mesh):
    sizes = dict(mesh.shape)
    return jax.shard_map(
        functools.partial(body, sizes["tok"], sizes["slot"]),
        mesh=mesh,
        in_specs=(P("tok", None), P("slot", None), P("slot", None, "tok"), P("slot", "tok", None)),
        out_specs=P(("tok", "slot"), None),
        check_vma=False,
    )
```

```python
import functools

import jax
import jax.numpy as jnp
from jax import lax
from jax.experimental import pallas as pl
from jax.experimental.pallas import tpu as pltpu
from jax.sharding import PartitionSpec as P

P_SIZE = 8
LANES = 128
TOKEN_CHUNKS = 4
BF = jnp.bfloat16
F32 = jnp.float32
VMEM = pl.BlockSpec(memory_space=pltpu.VMEM)
HBM = pl.BlockSpec(memory_space=pltpu.HBM)
MIB = 1 << 20
KERNEL_BYTES = 105 * MIB // 2


def sds(shape, dtype):
    return jax.ShapeDtypeStruct(shape, dtype)


def call(kernel, outs, in_specs, name, flops=0, moved=0, vmem=2 * MIB, **kw):
    return pl.pallas_call(
        kernel,
        out_shape=outs,
        in_specs=in_specs,
        out_specs=jax.tree.map(lambda _: VMEM, outs),
        name=name,
        compiler_params=pltpu.CompilerParams(vmem_limit_bytes=vmem),
        cost_estimate=pl.CostEstimate(flops=flops, bytes_accessed=moved, transcendentals=0),
        **kw,
    )


def lane_pack(rows, *columns):
    lane = lax.broadcasted_iota(jnp.int32, (rows, LANES), 1)
    out = jnp.zeros((rows, LANES), F32)
    for k, column in enumerate(columns):
        out = jnp.where(lane == k, column, out)
    return out


def write_state(num, top, tot, num_ref, st_ref, msg_ref):
    rows, d = num.shape
    num_ref[...] = num
    st_ref[...] = lane_pack(rows, top, tot)
    hi = tot.astype(BF).astype(F32)
    lo = (tot - hi).astype(BF).astype(F32)
    msg_ref[:, :d] = num.astype(BF)
    msg_ref[:, d:] = lane_pack(rows, top, hi, lo).astype(BF)


def dot_t(a, b):
    return lax.dot_general(a, b, (((1,), (1,)), ((), ())), preferred_element_type=F32)


def dispatch_kernel(chunks, sp_hbm, tok_hbm, tok_ref, flight_ref, num_ref, st_ref, msg_ref, sp_ref, sems):
    rows = flight_ref.shape[0]
    n = tok_ref.shape[0]
    step = n // chunks
    first = pltpu.make_async_copy(sp_hbm.at[pl.ds(0, rows)], sp_ref, sems.at[chunks])
    first.start()
    copies = []
    for c in range(chunks):
        part = pl.ds(c * step, step)
        copy = pltpu.make_async_copy(tok_hbm.at[part], tok_ref.at[part], sems.at[c])
        copy.start()
        copies.append(copy)
    first.wait()
    sp = sp_ref[...]
    for c, copy in enumerate(copies):
        copy.wait()
        flight_ref[:, c * step : (c + 1) * step] = dot_t(sp, tok_ref[c * step : (c + 1) * step, :])
    flight = flight_ref[...]
    top = jnp.max(flight, axis=1, keepdims=True).astype(BF).astype(F32)
    e = jnp.exp(flight - top)
    tot = jnp.sum(e, axis=1, keepdims=True)
    num = jnp.dot(e.astype(BF), tok_ref[...], preferred_element_type=F32)
    write_state(num, top, tot, num_ref, st_ref, msg_ref)


def merge(num_ref, st_ref, recvs):
    d = num_ref.shape[1]
    rs = [r[:, d:].astype(F32) for r in recvs]
    tops = [st_ref[:, 0:1]] + [r[:, 0:1] for r in rs]
    tots = [st_ref[:, 1:2]] + [r[:, 1:2] + r[:, 2:3] for r in rs]
    new = functools.reduce(jnp.maximum, tops)
    scales = [jnp.exp(t - new) for t in tops]
    num = num_ref[...] * scales[0]
    for r, s in zip(recvs, scales[1:]):
        num = num + r[:, :d].astype(F32) * s
    return num, new, sum(t * s for t, s in zip(tots, scales))


def merge_kernel(count, *refs):
    num_ref, st_ref, recvs, outs = refs[0], refs[1], refs[2 : 2 + count], refs[2 + count :]
    write_state(*merge(num_ref, st_ref, recvs), *outs)


def merge_last_kernel(*refs):
    num_ref, st_ref, recvs, out_ref = refs[0], refs[1], refs[2:-1], refs[-1]
    num, _, tot = merge(num_ref, st_ref, recvs)
    out_ref[...] = (num / tot).astype(BF)


def mlp_kernel(sizes, x_ref, win_ref, wout_ref, keep_ref, send_ref):
    x = x_ref[...].astype(F32)
    experts = win_ref.shape[0]
    width = keep_ref.shape[1]
    right = half_of(*sizes) == 1
    sent = []
    for e in range(experts):
        rows = slice(e * P_SIZE, (e + 1) * P_SIZE)
        pre = jnp.dot(x[rows].astype(BF), win_ref[e], preferred_element_type=F32)
        hidden = jax.nn.gelu(pre).astype(BF)
        out = jnp.dot(hidden, wout_ref[e], preferred_element_type=F32)
        a, b = out[:, :width], out[:, width:]
        keep_ref[rows, :] = jnp.where(right, b, a)
        sent.append(jnp.where(right, a, b))
    send_ref[...] = jnp.concatenate(sent, axis=0).astype(BF)


def add_kernel(*refs):
    keep_ref, recvs, (sum_ref, msg_ref) = refs[0], refs[1:-2], refs[-2:]
    total = keep_ref[...]
    for r in recvs:
        total = total + r[...].astype(F32)
    sum_ref[...] = total
    msg_ref[...] = total.astype(BF)


def stats_kernel(start, stop, step, sp_ref, tok_ref, *refs):
    n = tok_ref.shape[0]
    mo_ref, lo_ref = refs[-2:]
    if start == 0:
        m, l = jnp.full((8, n), -jnp.inf, F32), jnp.zeros((8, n), F32)
    else:
        m, l = refs[0][...], refs[1][...]
    tok = tok_ref[...]
    for r in range(start, stop, step):
        x = dot_t(sp_ref[r : r + step, :], tok).reshape(step // 8, 8, n)
        new = jnp.maximum(m, jnp.max(x, axis=0))
        l = l * jnp.exp(m - new) + jnp.sum(jnp.exp(x - new[None]), axis=0)
        m = new
    mo_ref[...] = m
    lo_ref[...] = l


def pack_kernel(flight_ref, m_ref, l_ref, out_ref):
    rows = flight_ref.shape[0]
    m, l = m_ref[...], l_ref[...]
    top = jnp.max(m, axis=0, keepdims=True)
    tot = jnp.sum(l * jnp.exp(m - top), axis=0, keepdims=True)
    sub = lax.broadcasted_iota(jnp.int32, m.shape, 0)
    tail = jnp.where(sub == 0, top, jnp.where(sub == 1, tot, 0.0))
    blocks, _, share = out_ref.shape
    for b in range(blocks):
        out_ref[b, :rows, :] = flight_ref[:, b * share : (b + 1) * share]
        out_ref[b, rows:, :] = tail[:, b * share : (b + 1) * share]


def weights_kernel(parts_ref, out_ref):
    blocks, rows, _ = parts_ref.shape
    rows -= 8
    tops = [parts_ref[b, rows : rows + 1, :] for b in range(blocks)]
    top = functools.reduce(jnp.maximum, tops)
    tot = sum(parts_ref[b, rows + 1 : rows + 2, :] * jnp.exp(t - top) for b, t in enumerate(tops))
    me = lax.axis_index("slot")
    w = [jnp.exp(parts_ref[me ^ k, :rows, :] - top) / tot for k in range(blocks)]
    out_ref[...] = jnp.concatenate(w, axis=0).T.astype(BF)


def combine_kernel(sizes, w_ref, mine_ref, recv_ref, out_ref):
    right = half_of(*sizes) == 1
    mine, recv = mine_ref[...], recv_ref[...]
    width = mine.shape[1]
    w = w_ref[...]
    out_ref[:, :width] = jnp.dot(w, jnp.where(right, recv, mine), preferred_element_type=F32).astype(BF)
    out_ref[:, width:] = jnp.dot(w, jnp.where(right, mine, recv), preferred_element_type=F32).astype(BF)


def half_of(n_tok, n_slot):
    bits = [lax.axis_index("tok") >> k for k in range(n_tok.bit_length() - 1)]
    bits += [lax.axis_index("slot") >> k for k in range(n_slot.bit_length() - 1)]
    return functools.reduce(lambda a, b: a ^ b, bits) & 1


def masks(bits):
    groups = []
    for at in range(0, len(bits), 2):
        pair = bits[at : at + 2]
        groups.append([pair[0]] if len(pair) == 1 else [pair[0], pair[1], pair[0] | pair[1]])
    return groups


def body(n_tok, n_slot, tokens, slot_params, w_in, w_out):
    n, d = tokens.shape
    experts, _, h = w_in.shape
    slots = slot_params.shape[0]
    rows = experts * P_SIZE
    width = d // 2
    share = n // n_slot
    def swap(x, tok, slot=0):
        pairs = [(i * n_slot + j, (i ^ tok) * n_slot + (j ^ slot)) for i in range(n_tok) for j in range(n_slot)]
        return lax.ppermute(x, ("tok", "slot"), pairs)

    def odd(mask):
        return mask.bit_count() & 1

    tok_groups = masks([1 << b for b in range(1, n_tok.bit_length() - 1)])
    slot_groups = masks([1 << b for b in range(n_slot.bit_length() - 1)])

    pieces = {"state": (), "at": 0}

    def stats(anchor, count):
        start, stop = pieces["at"], min(slots, pieces["at"] + count)
        if start == stop:
            return anchor
        *state, anchor = lax.optimization_barrier((*pieces["state"], anchor))
        state = call(
            functools.partial(stats_kernel, start, stop, min(256, stop - start)),
            [sds((8, n), F32)] * 2,
            [VMEM] * (2 + len(state)),
            "stats",
            flops=2 * (stop - start) * n * d,
            moved=4 * MIB,
            vmem=12 * MIB,
        )(slot_params, tok_v, *state)
        pieces.update(state=tuple(state), at=stop)
        return anchor

    def meet(values):
        k = len(pieces["state"])
        out = lax.optimization_barrier((*pieces["state"], *values))
        pieces.update(state=tuple(out[:k]))
        return list(out[k:])

    state = [sds((rows, d), F32), sds((rows, LANES), F32), sds((rows, d + LANES), BF)]
    chunks = TOKEN_CHUNKS
    tok_v, flight, num, st, msg = call(
        functools.partial(dispatch_kernel, chunks),
        [sds((n, d), BF), sds((rows, n), F32)] + state,
        [HBM, HBM],
        "dispatch",
        flops=4 * rows * n * d,
        moved=8 * MIB,
        vmem=KERNEL_BYTES - 2 * n * d,
        scratch_shapes=[pltpu.VMEM((rows, d), BF), pltpu.SemaphoreType.DMA((chunks + 1,))],
    )(slot_params, tokens)
    recvs = [swap(msg, 1)]
    msg = stats(msg, 256)
    for group in tok_groups:
        recvs = meet(recvs)
        num, st, msg = call(
            functools.partial(merge_kernel, len(recvs)), state, [VMEM] * (2 + len(recvs)), "merge", moved=8 * MIB
        )(num, st, *recvs)
        recvs = [swap(msg, mask | 1) for mask in group]
        msg = stats(msg, 768)
    recvs = meet(recvs)
    slot_in = call(merge_last_kernel, sds((rows, d), BF), [VMEM] * (2 + len(recvs)), "merge_last", moved=8 * MIB)(
        num, st, *recvs
    )

    def add(keep, recvs):
        outs = [sds((rows, width), F32), sds((rows, width), BF)]
        return call(add_kernel, outs, [VMEM] * (1 + len(recvs)), "add", moved=8 * MIB)(keep, *recvs)

    keep, send = call(
        functools.partial(mlp_kernel, (n_tok, n_slot)),
        [sds((rows, width), F32), sds((rows, width), BF)],
        [VMEM] * 3,
        "mlp",
        flops=4 * rows * d * h,
        moved=8 * MIB,
        vmem=4 * MIB,
    )(slot_in, w_in, w_out)
    recvs = [swap(send, 1)]
    send = stats(send, 256)
    for group in tok_groups:
        recvs = meet(recvs)
        keep, msg = add(keep, recvs)
        recvs = [swap(msg, mask | odd(mask)) for mask in group]
        msg = stats(msg, 768)
    stats(msg, slots)
    recvs = meet(recvs)
    _, msg = add(keep, recvs)
    outs = [msg]

    pack = call(pack_kernel, sds((n_slot, rows + 8, share), F32), [VMEM] * 3, "pack", moved=MIB)(
        flight, *pieces["state"]
    )
    parts = lax.all_to_all(pack, "slot", split_axis=0, concat_axis=0, tiled=True)
    weights = call(weights_kernel, sds((share, n_slot * rows), BF), [VMEM], "weights", vmem=4 * MIB)(
        parts
    )

    for group in slot_groups:
        have = outs[0] if len(outs) == 1 else jnp.concatenate(outs, axis=0)
        outs = [have] + [swap(have, odd(mask), mask) for mask in group]
    mine = jnp.concatenate(outs, axis=0)
    recv = swap(mine, 1)
    kernel = functools.partial(combine_kernel, (n_tok, n_slot))
    return call(kernel, sds((share, d), BF), [VMEM] * 3, "combine", vmem=8 * MIB)(weights, mine, recv)


def solution(mesh):
    sizes = dict(mesh.shape)
    return jax.shard_map(
        functools.partial(body, sizes["tok"], sizes["slot"]),
        mesh=mesh,
        in_specs=(P("tok", None), P("slot", None), P("slot", None, "tok"), P("slot", "tok", None)),
        out_specs=P(("tok", "slot"), None),
        check_vma=False,
    )
```
